64 devices in a mesh: rep: 8 (over x, y, core), dp: 8 (over z).
Axes of the slice: x: 2, y: 2, z: 8, core: 2. Of those that a mesh axis runs over, the one named last changes fastest.
The devices are a block of a 4x4x8 slice.
Arguments:
- x: bfloat16 [64, 2048, 512], P(('rep', 'dp')), parts along dimension 0
- dy: bfloat16 [64, 2048, 512], P(('rep', 'dp')), parts along dimension 0
- w_gate: bfloat16 [2, 512, 3072], replicated
- w_up: bfloat16 [2, 512, 3072], replicated
- w_down: bfloat16 [2, 3072, 512], replicated
- m_w_gate: float32 [2, 512, 3072], P(None, 'dp')
- m_w_up: float32 [2, 512, 3072], P(None, 'dp')
- m_w_down: float32 [2, 3072, 512], P(None, 'dp')
- v_w_gate: float32 [2, 512, 3072], P(None, 'dp')
- v_w_up: float32 [2, 512, 3072], P(None, 'dp')
- v_w_down: float32 [2, 3072, 512], P(None, 'dp')
Outputs:
- output 1: bfloat16 [16, 512, 3072], P('rep'), parts along dimension 0
- output 2: bfloat16 [16, 512, 3072], P('rep'), parts along dimension 0
- output 3: bfloat16 [16, 3072, 512], P('rep'), parts along dimension 0
- output 4: float32 [16, 512, 3072], P('rep', 'dp'), parts along dimension 0
- output 5: float32 [16, 512, 3072], P('rep', 'dp'), parts along dimension 0
- output 6: float32 [16, 3072, 512], P('rep', 'dp'), parts along dimension 0
- output 7: float32 [16, 512, 3072], P('rep', 'dp'), parts along dimension 0
- output 8: float32 [16, 512, 3072], P('rep', 'dp'), parts along dimension 0
- output 9: float32 [16, 3072, 512], P('rep', 'dp'), parts along dimension 0
There are 8 independent parts. The reference program is written for one: setup_inputs(seed, part) draws one part's arguments, and reference() takes and returns one part's arrays. A program takes and returns all parts, laid end to end along the dimension named above; an argument that names none is the same for every part.
All inputs are finite; a program needn't handle non-finite values.
Results may differ from the reference program's by a relative error of at most 0.022.
Values are sent between devices in bfloat16 or wider.
A program may use at most 768 MiB of HBM per device.

```python
import jax
import jax.numpy as jnp
from jax import lax

SEQUENCES = 8
TOKENS = 2048
D = 512
FF = 3072
LAYERS = 2
NAMES = ("w_gate", "w_up", "w_down")
SHAPES = {"w_gate": (LAYERS, D, FF), "w_up": (LAYERS, D, FF), "w_down": (LAYERS, FF, D)}


def bump(key, n, height):
    away = (jnp.arange(n, dtype=jnp.int32) - jax.random.randint(key, (), 0, n, jnp.int32)) % n
    return jnp.where(away < n // 8, height, 1.0)


def together(key, own, strength):
    shared = jax.random.normal(key, own.shape[1:], jnp.float32)
    return (own + strength * shared) * lax.rsqrt(1 + strength * strength)


def setup_inputs(seed: int = 0, part: int = 0) -> dict:
    kx, kdy, ka, kb, kz, kf, kh, kl, *keys = jax.random.split(jax.random.key(seed), 8 + 3 * len(NAMES))
    kx, kdy, ka, kb = (jax.random.fold_in(k, part) for k in (kx, kdy, ka, kb))
    kw, km, kv = (keys[i::3] for i in range(3))
    shape = (SEQUENCES, TOKENS, D)
    much_x, much_dy = jax.random.uniform(kz, (2,), jnp.float32, 0.0, 1.0)
    loud = 2.0 ** jax.random.uniform(jax.random.fold_in(kz, 1), (), jnp.float32, -1.0, 2.0)
    layers = 2.0 ** jax.random.uniform(kl, (LAYERS, 1, 1), jnp.float32, -1.0, 1.0)
    x = together(ka, jax.random.normal(kx, shape, jnp.float32), much_x) * bump(kf, D, 4.0)
    dy = together(kb, jax.random.normal(kdy, shape, jnp.float32), much_dy)
    drawn = {"x": x.astype(jnp.bfloat16), "dy": (loud * dy * (SEQUENCES * TOKENS) ** -0.5).astype(jnp.bfloat16)}
    for key, name in zip(kw, NAMES, strict=True):
        w = jax.random.normal(key, SHAPES[name], jnp.float32) * SHAPES[name][1] ** -0.5
        drawn[name] = (w * {"w_gate": 1.0, "w_up": bump(kh, FF, 4.0), "w_down": layers}[name]).astype(jnp.bfloat16)
    for key, name in zip(km, NAMES, strict=True):
        drawn[f"m_{name}"] = 0.1 * jax.random.normal(key, SHAPES[name], jnp.float32)
    for key, name in zip(kv, NAMES, strict=True):
        drawn[f"v_{name}"] = jax.random.uniform(key, SHAPES[name], jnp.float32, 0.005, 0.015)
    return drawn


def matmul(a, w):
    return jnp.dot(a, w, preferred_element_type=jnp.float32).astype(jnp.bfloat16)


def normed(h):
    wide = h.astype(jnp.float32)
    scale = lax.rsqrt(jnp.mean(wide**2, -1, keepdims=True) + 1e-6)
    return (wide * scale).astype(jnp.bfloat16)


def layer(h, w):
    a = normed(h)
    gate = jnp.dot(a, w["w_gate"], preferred_element_type=jnp.float32)
    up = jnp.dot(a, w["w_up"], preferred_element_type=jnp.float32)
    return h + matmul((jax.nn.silu(gate) * up).astype(jnp.bfloat16), w["w_down"])


def adamw(w, m, v, g):
    m = 0.9 * m + 0.1 * g
    v = 0.95 * v + 0.05 * g * g
    step = m * lax.rsqrt(v + 1e-8) + 0.1 * w
    return (w - 0.02 * step).astype(jnp.bfloat16), m, v


def stack(weights, h):
    return lax.scan(lambda h, w: (layer(h, w), None), h, weights)[0]


def reference(x, dy, w_gate, w_up, w_down, m_w_gate, m_w_up, m_w_down, v_w_gate, v_w_up, v_w_down):
    weights = dict(zip(NAMES, (w_gate, w_up, w_down), strict=True))

    def take(so_far, sequence):
        h, by_y = sequence
        _, back = jax.vjp(lambda w: stack(w, h), weights)
        return jax.tree.map(lambda total, term: total + term.astype(jnp.float32), so_far, back(by_y)[0]), None

    none_yet = {name: jnp.zeros(w.shape, jnp.float32) for name, w in weights.items()}
    by_weights, _ = lax.scan(take, none_yet, (x, dy))
    gradients = [by_weights[name].astype(jnp.bfloat16).astype(jnp.float32) for name in NAMES]
    new = [
        adamw(w.astype(jnp.float32), m, v, g)
        for w, m, v, g in zip((w_gate, w_up, w_down), (m_w_gate, m_w_up, m_w_down), (v_w_gate, v_w_up, v_w_down), gradients, strict=True)
    ]
    return tuple(one[which] for which in range(3) for one in new)
```

```python
import jax
import jax.numpy as jnp
from jax import lax
from jax.sharding import PartitionSpec as P

F32 = jnp.float32
BF16 = jnp.bfloat16


def dot(a, b, dims=((1,), (0,))):
    return lax.dot_general(a, b, (dims, ((), ())), preferred_element_type=F32)


def normed(h):
    wide = h.astype(F32)
    scale = lax.rsqrt(jnp.mean(wide**2, -1, keepdims=True) + 1e-6)
    return (wide * scale).astype(BF16), scale


def adamw(w, m, v, g):
    m = 0.9 * m + 0.1 * g
    v = 0.95 * v + 0.05 * g * g
    step = m * lax.rsqrt(v + 1e-8) + 0.1 * w
    return (w - 0.02 * step).astype(BF16), m, v


def device_step(x, dy, w_gate, w_up, w_down, *moments):
    m, v = moments[:3], moments[3:]
    layers = w_gate.shape[0]
    me = lax.axis_index("dp")
    h = x[0]
    saved = []
    for n in range(layers):
        a, scale = normed(h)
        gate = dot(a, w_gate[n])
        up = dot(a, w_up[n])
        sig = jax.nn.sigmoid(gate)
        p = (gate * sig * up).astype(BF16)
        saved.append((h, a, scale, gate, up, sig, p))
        if n < layers - 1:
            h = h + dot(p, w_down[n]).astype(BF16)
    ct = dy[0]
    sums = [None] * layers
    for n in reversed(range(layers)):
        h, a, scale, gate, up, sig, p = saved[n]
        d_down = dot(p, ct, ((0,), (0,))).astype(BF16)
        dp = dot(ct, w_down[n], ((1,), (1,))).astype(BF16).astype(F32)
        d_up_in = (dp * gate * sig).astype(BF16)
        d_gate_in = (dp * up * (sig + gate * sig * (1 - sig))).astype(BF16)
        d_gate = dot(a, d_gate_in, ((0,), (0,))).astype(BF16)
        d_up = dot(a, d_up_in, ((0,), (0,))).astype(BF16)
        sums[n] = [lax.psum_scatter(g, "dp", scatter_dimension=0, tiled=True) for g in (d_gate, d_up, d_down)]
        if n > 0:
            da = dot(d_gate_in, w_gate[n], ((1,), (1,))).astype(BF16) + dot(d_up_in, w_up[n], ((1,), (1,))).astype(BF16)
            da = da.astype(F32)
            wide = h.astype(F32)
            inner = jnp.mean(da * wide, -1, keepdims=True)
            ct = ct + (da * scale - wide * (scale**3 * inner)).astype(BF16)
    new = []
    for i, w in enumerate((w_gate, w_up, w_down)):
        rows = m[i].shape[1]
        own = lax.dynamic_slice_in_dim(w, me * rows, rows, 1).astype(F32)
        g = jnp.stack([sums[n][i] for n in range(layers)]).astype(F32)
        new.append(adamw(own, m[i], v[i], g))
    gathered = tuple(lax.all_gather(one[0], "dp", axis=1, tiled=True) for one in new)
    return gathered + tuple(one[which] for which in (1, 2) for one in new)


def solution(mesh):
    whole, rows, seq = P(None, None, None), P(None, "dp", None), P(("rep", "dp"), None, None)
    return jax.shard_map(
        device_step,
        mesh=mesh,
        in_specs=(seq, seq) + (whole,) * 3 + (rows,) * 6,
        out_specs=(P("rep", None, None),) * 3 + (P("rep", "dp", None),) * 6,
        check_vma=False,
    )
```

```python
import functools

import jax
import jax.numpy as jnp
from jax import lax
from jax.experimental import pallas as pl
from jax.experimental.pallas import tpu as pltpu
from jax.sharding import PartitionSpec as P

F32 = jnp.float32
BF16 = jnp.bfloat16
MESH = pl.DeviceIdType.MESH
STRIP = 128
WIDE = 2 * STRIP
SLOTS = 6
AG_FROM = 8
COMM = True
COMPUTE = True


def dot(a, b, dims=((1,), (0,))):
    return lax.dot_general(a, b, (dims, ((), ())), preferred_element_type=F32)


def aligned(i, m):
    return pl.multiple_of(i, m)


def kernel(
    n, x, dy, wg, wu, wd, mg, mu, md, vg, vu, vd,
    og, ou, od, omg, omu, omd, ovg, ovu, ovd,
    h_ref, a_ref, at_ref, ct_ref, acc_ref, p_ref, dgu_ref, wgu_buf, wd_buf,
    g_gu, g_dn, land_gu, land_dn, m_gu, v_gu, m_dn, v_dn, own_gu, own_dn,
    w_sem, in_sem, out_sem, gu_send, gu_recv, dn_send, dn_recv, ag_send, ag_recv,
):
    tokens, d = h_ref.shape
    layers, _, ff = wg.shape
    rows = d // n
    share = ff // n
    per_layer = ff // WIDE
    per_chunk = n // 2
    chunks = per_layer // per_chunk
    tiles = layers * per_layer
    half = STRIP // 2
    block = tokens // 4
    me, rep = lax.axis_index("dp"), lax.axis_index("rep")
    right, left = lax.rem(me + 1, n), lax.rem(me + n - 1, n)
    to = (right, left)

    def owner(direction, hop):
        return lax.rem(me + n - 1 - hop, n) if direction == 0 else lax.rem(me + 1 + hop, n)

    def holder(direction, hop):
        return lax.rem(me + n - hop, n) if direction == 0 else lax.rem(me + hop, n)

    def place(t):
        tt = lax.rem(t, per_layer)
        return layers - 1 - lax.div(t, per_layer), lax.div(tt, per_chunk), lax.rem(tt, per_chunk)

    def strips(j, i):
        return [aligned((2 * i + k) * share + STRIP * j, STRIP) for k in range(2)]

    def tile_copies(g):
        lay = lax.rem(lax.div(g, per_layer), 2)
        tt = lax.rem(g, per_layer)
        cols = strips(lax.div(tt, per_chunk), lax.rem(tt, per_chunk))
        slot = lax.rem(g, 2)
        out = []
        for k, col in enumerate(cols):
            strip = pl.ds(col, STRIP)
            for q, w in enumerate((wg, wu)):
                out.append((w.at[lay, :, strip], wgu_buf.at[slot, :, pl.ds(q * WIDE + k * STRIP, STRIP)]))
            out.append((wd.at[lay, strip], wd_buf.at[slot, pl.ds(k * STRIP, STRIP)]))
        return [pltpu.make_async_copy(a, b, w_sem.at[slot, k]) for k, (a, b) in enumerate(out)]

    def fetch(g):
        for c in tile_copies(g):
            c.start()

    def fetched(g):
        for c in tile_copies(g):
            c.wait()

    load_x = pltpu.make_async_copy(x.at[0], h_ref, in_sem.at[0])
    load_dy = pltpu.make_async_copy(dy.at[0], ct_ref, in_sem.at[1])
    moments = [
        pltpu.make_async_copy(a, b, in_sem.at[2 + k])
        for k, (a, b) in enumerate(
            ((mg, m_gu.at[0]), (mu, m_gu.at[1]), (vg, v_gu.at[0]), (vu, v_gu.at[1]), (md, m_dn), (vd, v_dn),
             (wg.at[:, pl.ds(aligned(me * rows, rows), rows)], own_gu.at[0]),
             (wu.at[:, pl.ds(aligned(me * rows, rows), rows)], own_gu.at[1]),
             (wd.at[:, pl.ds(aligned(me * share, share), share)], own_dn))
        )
    ]

    def results(lay):
        mine, down = pl.ds(aligned(me * rows, rows), rows), pl.ds(aligned(me * share, share), share)
        pairs = (
            (m_gu.at[0, lay], omg.at[lay]), (m_gu.at[1, lay], omu.at[lay]), (m_dn.at[lay], omd.at[lay]),
            (v_gu.at[0, lay], ovg.at[lay]), (v_gu.at[1, lay], ovu.at[lay]), (v_dn.at[lay], ovd.at[lay]),
            (own_gu.at[0, lay], og.at[lay, mine]), (own_gu.at[1, lay], ou.at[lay, mine]), (own_dn.at[lay], od.at[lay, down]),
        )
        return [pltpu.make_async_copy(a, b, out_sem.at[lay, k]) for k, (a, b) in enumerate(pairs)]

    barrier = pltpu.get_barrier_semaphore()
    for other in to:
        pl.semaphore_signal(barrier, inc=1, device_id=(rep, other), device_id_type=MESH)
    load_x.start()
    fetch(0)
    load_dy.start()
    for c in moments:
        c.start()
    pl.semaphore_wait(barrier, 2)

    def remote(src, dst, send, recv, direction):
        return pltpu.make_async_remote_copy(
            src_ref=src, dst_ref=dst, send_sem=send, recv_sem=recv, device_id=(rep, to[direction]), device_id_type=MESH
        )

    def adam(w, m, v, g):
        g = g.astype(F32)
        m = 0.9 * m + 0.1 * g
        v = 0.95 * v + 0.05 * g * g
        step = m * lax.rsqrt(v + 1e-8) + 0.1 * w
        return (w - 0.02 * step).astype(BF16), m, v

    def gu_copy(u, s, direction):
        slot = lax.rem(u, SLOTS)
        if s == 0:
            src = g_gu.at[slot, direction, pl.ds(aligned(owner(direction, 0) * rows, rows), rows)]
        else:
            src = land_gu.at[slot, s - 1, direction]
        return remote(src, land_gu.at[slot, s, direction], gu_send.at[slot, direction], gu_recv.at[slot, s, direction], direction)

    def gu_event(u, s):
        slot = lax.rem(u, SLOTS)
        if s > 0:
            for e in range(2):
                before = gu_copy(u, s - 1, e)
                before.wait_send()
                before.wait_recv()
                mine = g_gu[slot, e, pl.ds(aligned(owner(e, s) * rows, rows), rows)]
                total = (land_gu[slot, s - 1, e].astype(F32) + mine.astype(F32)).astype(BF16)
                if s < n - 1:
                    land_gu[slot, s - 1, e] = total
                else:
                    lay, j, i = place(u)
                    for k, col in enumerate(strips(j, i)):
                        strip = pl.ds(col, STRIP)
                        new, m, v = adam(
                            own_gu[e, lay, :, strip].astype(F32), m_gu[e, lay, :, strip], v_gu[e, lay, :, strip],
                            total[:, k * STRIP : (k + 1) * STRIP],
                        )
                        own_gu[e, lay, :, strip] = new
                        m_gu[e, lay, :, strip] = m
                        v_gu[e, lay, :, strip] = v
        if s < n - 1:
            for e in range(2):
                gu_copy(u, s, e).start()

    def dn_first(c, e):
        slot = lax.rem(c, 2)
        src = g_dn.at[slot, owner(e, 0), pl.ds(e * half, half)]
        return remote(src, land_dn.at[slot, 0, e], dn_send.at[slot, e], dn_recv.at[slot, 0, e], e)

    def dn_next(c, s, e):
        slot = lax.rem(c, 2)
        return remote(land_dn.at[slot, s - 1, e], land_dn.at[slot, s, e], dn_send.at[slot, e], dn_recv.at[slot, s, e], e)

    def dn_event(c, s):
        slot = lax.rem(c, 2)

        @pl.when(s == 0)
        def _():
            for e in range(2):
                dn_first(c, e).start()

        @pl.when(s > 0)
        def _():
            for e in range(2):
                before = remote(
                    land_dn.at[slot, s - 1, e], land_dn.at[slot, s - 1, e], dn_send.at[slot, e], dn_recv.at[slot, s - 1, e], e
                )
                before.wait_send()
                before.wait_recv()
                mine = g_dn[slot, owner(e, s), pl.ds(e * half, half)]
                land_dn[slot, s - 1, e] = (land_dn[slot, s - 1, e].astype(F32) + mine.astype(F32)).astype(BF16)

            @pl.when(s < n - 1)
            def _():
                for e in range(2):
                    dn_next(c, s, e).start()

            @pl.when(s == n - 1)
            def _():
                lay, j, _ = place(c * per_chunk)
                for e in range(2):
                    r = pl.ds(aligned(STRIP * j + e * half, half), half)
                    new, m, v = adam(own_dn[lay, r].astype(F32), m_dn[lay, r], v_dn[lay, r], land_dn[slot, n - 2, e])
                    own_dn[lay, r] = new
                    m_dn[lay, r] = m
                    v_dn[lay, r] = v

    def ag_start(c, h, first):
        lay, j, _ = place(c * per_chunk)
        for e in range(2):
            who = holder(e, h)
            r = pl.ds(aligned(who * rows, rows), rows)
            out = (og, ou)[e]
            send, recv = ag_send.at[c, e], ag_recv.at[c, h, e]

            def strip_copy(i, _):
                strip = pl.ds(aligned(i * share + STRIP * j, STRIP), STRIP)
                there = out.at[lay, r, strip]
                remote(own_gu.at[e, lay, :, strip] if first else there, there, send, recv, e).start()
                return 0

            lax.fori_loop(0, n, strip_copy, 0)
            there = od.at[lay, pl.ds(aligned(who * share + STRIP * j + e * half, half), half)]
            src = own_dn.at[lay, pl.ds(aligned(STRIP * j + e * half, half), half)] if first else there
            remote(src, there, send, recv, e).start()

    def ag_wait(c, h):
        sent = (n * rows * STRIP + half * d) // d
        for e in range(2):
            all_of_it = od.at[0, pl.ds(0, sent)]
            before = remote(all_of_it, all_of_it, ag_send.at[c, e], ag_recv.at[c, h, e], e)
            before.wait_send()
            before.wait_recv()

    def ag_event(c, h):
        @pl.when(h == 0)
        def _():
            ag_start(c, 0, True)

        @pl.when(h > 0)
        def _():
            ag_wait(c, h - 1)

            @pl.when(h < n - 1)
            def _():
                ag_start(c, h, False)

    def pump(t, part):
        if not COMM:
            return
        for back in range(1, per_chunk + 1):
            s = 2 * (back - 1) + part
            if s > n - 1:
                continue

            @pl.when((t >= back) & (t - back < tiles))
            def _():
                gu_event(t - back, s)

        @pl.when(t >= per_chunk)
        def _():
            dn_event(lax.div(t, per_chunk) - 1, 2 * lax.rem(t, per_chunk) + part)

        if part == 1:

            @pl.when(t >= AG_FROM)
            def _():
                ag_event(lax.div(t - AG_FROM, n), lax.rem(t - AG_FROM, n))

            @pl.when(t == 4 * per_chunk)
            def _():
                for c in results(layers - 1):
                    c.start()

    def normalise(b, _):
        r = pl.ds(aligned(b * 256, 256), 256)
        wide = h_ref[r].astype(F32)
        scale = lax.rsqrt(jnp.mean(wide * wide, -1, keepdims=True) + 1e-6)
        a = wide * scale
        a_ref[r] = a.astype(BF16)
        at_ref[:, r] = a.T.astype(BF16)
        return 0

    def gates(r, slot):
        gu = dot(a_ref[r], wgu_buf[slot])
        gate, up = gu[:, :WIDE], gu[:, WIDE:]
        sig = jax.nn.sigmoid(gate)
        return gate * sig, up, sig

    load_x.wait()
    lax.fori_loop(0, tokens // 256, normalise, 0)
    acc_ref[...] = jnp.zeros_like(acc_ref)

    def forward(g, _):
        slot = lax.rem(g, 2)
        fetch(g + 1)
        fetched(g)
        for b in range(4):
            r = pl.ds(b * block, block)
            silu, up, _ = gates(r, slot)
            acc_ref[r] += dot((silu * up).astype(BF16), wd_buf[slot])
        return 0

    if COMPUTE:
        lax.fori_loop(0, per_layer, forward, 0)

    def join(b, _):
        r = pl.ds(aligned(b * 256, 256), 256)
        h_ref[r] = h_ref[r] + acc_ref[r].astype(BF16)
        acc_ref[r] = jnp.zeros((256, d), F32)
        return normalise(b, 0)

    lax.fori_loop(0, tokens // 256, join, 0)
    load_dy.wait()
    for c in moments:
        c.wait()

    def backward(t, _, with_da, last):
        g = t + per_layer
        slot = lax.rem(g, 2)
        if COMPUTE:
            if last:

                @pl.when(t < tiles - 1)
                def _():
                    fetch(g + 1)
            else:
                fetch(g + 1)
            fetched(g)
        lay, j, i = place(t)
        for b in range(4 if COMPUTE else 0):
            r = pl.ds(b * block, block)
            silu, up, sig = gates(r, slot)
            dp = dot(ct_ref[r], wd_buf[slot], ((1,), (1,))).astype(BF16).astype(F32)
            p_ref[r] = (silu * up).astype(BF16)
            dgu_ref[r, WIDE:] = (dp * silu).astype(BF16)
            dgu_ref[r, :WIDE] = (dp * up * (sig + silu * (1 - sig))).astype(BF16)
            if with_da:
                acc_ref[r] += dot(dgu_ref[r], wgu_buf[slot], ((1,), (1,)))
            if b == 0:
                pump(t, 0)
        if not COMPUTE:
            pump(t, 0)
        if COMPUTE:
            grads = dot(p_ref[...], ct_ref[...], ((0,), (0,))).astype(BF16)
            dslot = lax.rem(lax.div(t, per_chunk), 2)
            for k in range(2):
                g_dn[dslot, 2 * i + k] = grads[k * STRIP : (k + 1) * STRIP]
        pump(t, 1)
        if COMPUTE:
            grads = dot(at_ref[...], dgu_ref[...]).astype(BF16)
            for e in range(2):
                g_gu[lax.rem(t, SLOTS), e] = grads[:, e * WIDE : (e + 1) * WIDE]
        return 0

    lax.fori_loop(0, per_layer, functools.partial(backward, with_da=True, last=False), 0)

    def turn(b, _):
        r = pl.ds(aligned(b * 256, 256), 256)
        wide = h_ref[r].astype(F32)
        scale = lax.rsqrt(jnp.mean(wide * wide, -1, keepdims=True) + 1e-6)
        da = acc_ref[r].astype(BF16).astype(F32)
        inner = jnp.mean(da * wide, -1, keepdims=True)
        ct_ref[r] = ct_ref[r] + (da * scale - wide * (scale * scale * scale * inner)).astype(BF16)
        return 0

    lax.fori_loop(0, tokens // 256, turn, 0)
    load_x.start()
    load_x.wait()
    lax.fori_loop(0, tokens // 256, normalise, 0)
    lax.fori_loop(per_layer, tiles, functools.partial(backward, with_da=False, last=True), 0)

    def drain(t, _):
        pump(t, 0)
        pump(t, 1)
        return 0

    lax.fori_loop(tiles, tiles + per_chunk, drain, 0)
    for c in results(0):
        c.start()
    if COMM:
        done = tiles + per_chunk - AG_FROM
        part, begun = done % n, done // n

        def rest(h, _):
            for c in range(begun + (part > 0), layers * chunks):
                ag_event(c, h)
            if part:

                @pl.when(h + part < n)
                def _():
                    ag_event(begun, h + part)

            return 0

        lax.fori_loop(0, n, rest, 0)
    else:
        for c in results(layers - 1):
            c.start()
    for lay in range(layers):
        for c in results(lay):
            c.wait()


def device_step(n, x, dy, *arrays):
    w, m, v = (arrays[i : i + 3] for i in (0, 3, 6))
    layers, d, ff = w[0].shape
    tokens = x.shape[1]
    rows, share = d // n, ff // n
    hops, chunks = n - 1, share // STRIP * layers
    anywhere = pl.BlockSpec(memory_space=pl.ANY)
    dma = pltpu.SemaphoreType.DMA
    return pl.pallas_call(
        functools.partial(kernel, n),
        name="step",
        out_shape=[jax.ShapeDtypeStruct(a.shape, a.dtype) for a in (*w, *m, *v)],
        in_specs=[anywhere] * 11,
        out_specs=[anywhere] * 9,
        scratch_shapes=[
            pltpu.VMEM((tokens, d), BF16),
            pltpu.VMEM((tokens, d), BF16),
            pltpu.VMEM((d, tokens), BF16),
            pltpu.VMEM((tokens, d), BF16),
            pltpu.VMEM((tokens, d), F32),
            pltpu.VMEM((tokens, WIDE), BF16),
            pltpu.VMEM((tokens, 2 * WIDE), BF16),
            pltpu.VMEM((2, d, 2 * WIDE), BF16),
            pltpu.VMEM((2, WIDE, d), BF16),
            pltpu.VMEM((SLOTS, 2, d, WIDE), BF16),
            pltpu.VMEM((2, n, STRIP, d), BF16),
            pltpu.VMEM((SLOTS, hops, 2, rows, WIDE), BF16),
            pltpu.VMEM((2, hops, 2, STRIP // 2, d), BF16),
            pltpu.VMEM((2, layers, rows, ff), F32),
            pltpu.VMEM((2, layers, rows, ff), F32),
            pltpu.VMEM((layers, share, d), F32),
            pltpu.VMEM((layers, share, d), F32),
            pltpu.VMEM((2, layers, rows, ff), BF16),
            pltpu.VMEM((layers, share, d), BF16),
            dma((2, 6)),
            dma((11,)),
            dma((layers, 9)),
            dma((SLOTS, 2)),
            dma((SLOTS, hops, 2)),
            dma((2, 2)),
            dma((2, hops, 2)),
            dma((chunks, 2)),
            dma((chunks, hops, 2)),
        ],
        compiler_params=pltpu.CompilerParams(collective_id=0, has_side_effects=True, vmem_limit_bytes=63 * 2**20),
    )(x, dy, *arrays)


def solution(mesh):
    whole, rows, seq = P(None, None, None), P(None, "dp", None), P(("rep", "dp"), None, None)
    return jax.shard_map(
        functools.partial(device_step, mesh.shape["dp"]),
        mesh=mesh,
        in_specs=(seq, seq) + (whole,) * 3 + (rows,) * 6,
        out_specs=(P("rep", None, None),) * 3 + (P("rep", "dp", None),) * 6,
        check_vma=False,
    )
```

```python
import functools

import jax
import jax.numpy as jnp
from jax import lax
from jax.experimental import pallas as pl
from jax.experimental.pallas import tpu as pltpu
from jax.sharding import PartitionSpec as P

F32 = jnp.float32
BF16 = jnp.bfloat16
MESH = pl.DeviceIdType.MESH
STRIP = 128
WIDE = 2 * STRIP
SLOTS = 6
DN_SLOTS = 3
DRAIN_UNITS = 4
LAG = 4
GROUPS = ((0, 1, 2, 3), (4, 5), (6, 7, 8, 9, 10))
STEPS = len(GROUPS)
GU_FROM = 2
DN_FROM = 3


def dot(a, b, dims=((1,), (0,))):
    return lax.dot_general(a, b, (dims, ((), ())), preferred_element_type=F32)


def aligned(i, m):
    return pl.multiple_of(i, m)


def kernel(
    n, x, dy, wg, wu, wd, mg, mu, md, vg, vu, vd,
    og, ou, od, omg, omu, omd, ovg, ovu, ovd,
    h_ref, a_ref, at_ref, ct_ref, acc_ref, p_ref, dgu_ref, wgu_buf, wd_buf,
    g_gu, g_dn, land_gu, land_dn,
    w_sem, in_sem, gu_send, gu_recv, dn_send, dn_recv, ag_send, ag_recv,
):
    tokens, d = h_ref.shape
    layers, _, ff = wg.shape
    rows = d // n
    share = ff // n
    per_layer = ff // WIDE
    per_chunk = n // 2
    chunks = layers * per_layer // per_chunk
    tiles = layers * per_layer
    half = STRIP // 2
    block = tokens // 4
    me, rep = lax.axis_index("dp"), lax.axis_index("rep")
    right, left = lax.rem(me + 1, n), lax.rem(me + n - 1, n)
    to = (right, left)

    longer = n // 2

    def length(e, direction):
        return longer if e == direction else n - 1 - longer

    def owner(e, direction, hop):
        away = length(e, direction) - hop
        return lax.rem(me + away, n) if direction == 0 else lax.rem(me + n - away, n)

    def holder(direction, hop):
        return lax.rem(me + n - hop, n) if direction == 0 else lax.rem(me + hop, n)

    def place(t):
        tt = lax.rem(t, per_layer)
        return layers - 1 - lax.div(t, per_layer), lax.div(tt, per_chunk), lax.rem(tt, per_chunk)

    def strips(j, i):
        return [aligned((2 * i + k) * share + STRIP * j, STRIP) for k in range(2)]

    def tile_copies(g):
        lay = lax.rem(lax.div(g, per_layer), 2)
        tt = lax.rem(g, per_layer)
        cols = strips(lax.div(tt, per_chunk), lax.rem(tt, per_chunk))
        slot = lax.rem(g, 2)
        out = []
        for k, col in enumerate(cols):
            strip = pl.ds(col, STRIP)
            for q, w in enumerate((wg, wu)):
                out.append((w.at[lay, :, strip], wgu_buf.at[slot, :, pl.ds(q * WIDE + k * STRIP, STRIP)]))
            out.append((wd.at[lay, strip], wd_buf.at[slot, pl.ds(k * STRIP, STRIP)]))
        return [pltpu.make_async_copy(a, b, w_sem.at[slot, k]) for k, (a, b) in enumerate(out)]

    def fetch(g):
        for c in tile_copies(g):
            c.start()

    def fetched(g):
        for c in tile_copies(g):
            c.wait()

    load_x = pltpu.make_async_copy(x.at[0], h_ref, in_sem.at[0])
    load_dy = pltpu.make_async_copy(dy.at[0], ct_ref, in_sem.at[1])
    my_rows, my_share = pl.ds(aligned(me * rows, rows), rows), pl.ds(aligned(me * share, share), share)
    moments = [
        pltpu.make_async_copy(a, b, in_sem.at[2 + k])
        for k, (a, b) in enumerate(
            ((mg, omg), (mu, omu), (md, omd), (vg, ovg), (vu, ovu), (vd, ovd),
             (wg.at[:, my_rows], og.at[:, my_rows]), (wu.at[:, my_rows], ou.at[:, my_rows]), (wd.at[:, my_share], od.at[:, my_share]))
        )
    ]

    barrier = pltpu.get_barrier_semaphore()
    for other in to:
        pl.semaphore_signal(barrier, inc=1, device_id=(rep, other), device_id_type=MESH)
    load_x.start()
    fetch(0)
    load_dy.start()

    def remote(src, dst, send, recv, direction):
        return pltpu.make_async_remote_copy(
            src_ref=src, dst_ref=dst, send_sem=send, recv_sem=recv, device_id=(rep, to[direction]), device_id_type=MESH
        )

    def adam(w, m, v, g):
        g = g.astype(F32)
        m = 0.9 * m + 0.1 * g
        v = 0.95 * v + 0.05 * g * g
        step = m * lax.rsqrt(v + 1e-8) + 0.1 * w
        return (w - 0.02 * step).astype(BF16), m, v

    def sum_event(hop, own, land, send, recv, update):
        def copy(e, direction, h):
            src = own(e, owner(e, direction, 0)) if h == 0 else land.at[e, direction, h - 1]
            return remote(src, land.at[e, direction, h], send.at[e, direction], recv.at[e, direction, h], direction)

        def ended(e, direction, h):
            before = copy(e, direction, h)
            before.wait_send()
            before.wait_recv()
            return land[e, direction, h].astype(F32)

        if hop == longer:
            for e in range(2):
                whole = own(e, me)[...].astype(F32)
                for direction in range(2):
                    whole += ended(e, direction, length(e, direction) - 1)
                update(e, whole.astype(BF16))
            return
        ready = []
        for e, direction in ((0, 0), (1, 1), (1, 0), (0, 1)):
            if hop >= length(e, direction):
                continue
            if hop > 0:
                mine = own(e, owner(e, direction, hop))[...].astype(F32)
                land[e, direction, hop - 1] = (ended(e, direction, hop - 1) + mine).astype(BF16)
            ready.append(copy(e, direction, hop))
            if len(ready) > 1:
                ready[-2].start()
        ready[-1].start()

    def gu_event(u, hop):
        slot = lax.rem(u, SLOTS)
        lay, j, i = place(u)

        def update(e, g):
            w, m, v = ((og, omg, ovg), (ou, omu, ovu))[e]
            for k, col in enumerate(strips(j, i)):
                strip = pl.ds(col, STRIP)
                w[lay, my_rows, strip], m[lay, :, strip], v[lay, :, strip] = adam(
                    w[lay, my_rows, strip].astype(F32), m[lay, :, strip], v[lay, :, strip], g[:, k * STRIP : (k + 1) * STRIP]
                )

        def own(e, who):
            return g_gu.at[slot, e, pl.ds(aligned(who * rows, rows), rows)]

        sum_event(hop, own, land_gu.at[slot], gu_send.at[slot], gu_recv.at[slot], update)

    def dn_event(c, hop):
        slot = lax.rem(c, DN_SLOTS)
        lay, j, _ = place(c * per_chunk)

        def update(e, g):
            r = pl.ds(aligned(STRIP * j + e * half, half), half)
            mine = pl.ds(aligned(me * share + STRIP * j + e * half, half), half)
            od[lay, mine], omd[lay, r], ovd[lay, r] = adam(od[lay, mine].astype(F32), omd[lay, r], ovd[lay, r], g)

        def own(e, who):
            return g_dn.at[slot, who, pl.ds(e * half, half)]

        sum_event(hop, own, land_dn.at[slot], dn_send.at[slot], dn_recv.at[slot], update)

    def new_copies(c, e, direction, h):
        lay, j, _ = place(c * per_chunk)
        who = holder(direction, h)
        send, recv = ag_send.at[c, e, direction], ag_recv.at[c, e, direction, h]
        out, r = (og, ou)[e], pl.ds(aligned(who * rows, rows), rows)

        for i in range(n):
            there = out.at[lay, r, pl.ds(aligned(i * share + STRIP * j, STRIP), STRIP)]
            remote(there, there, send, recv, direction).start()
        there = od.at[lay, pl.ds(aligned(who * share + STRIP * j + e * half, half), half)]
        remote(there, there, send, recv, direction).start()

    def new_ended(c, e, direction, h):
        sent = (n * rows * STRIP + half * d) // d
        all_of_it = od.at[0, pl.ds(0, sent)]
        before = remote(all_of_it, all_of_it, ag_send.at[c, e, direction], ag_recv.at[c, e, direction, h], direction)
        before.wait_send()
        before.wait_recv()

    def ag_event(unit, hop):
        c = lax.div(unit, 2)
        for e in range(2):

            @pl.when(lax.rem(unit, 2) == e)
            def _():
                for direction in range(2):

                    @pl.when((hop > 0) & (hop < length(e, direction)))
                    def _():
                        new_ended(c, e, direction, hop - 1)

                for direction in range(2):

                    @pl.when(hop < length(e, direction))
                    def _():
                        new_copies(c, e, direction, hop)

    def pump(t, step):
        for hop in range(longer + 1):
            since, due = divmod(GU_FROM + LAG * hop, STEPS)
            if due == step:

                @pl.when((t >= since) & (t < tiles + since))
                def _():
                    gu_event(t - since, hop)

            since, due = divmod(DN_FROM + LAG * hop, STEPS)
            if due == step:

                @pl.when((t >= since) & (t < tiles + since) & (lax.rem(t - since + 1, per_chunk) == 0))
                def _():
                    dn_event(lax.div(t - since, per_chunk), hop)

    def normalise(b, _, turned=True):
        r = pl.ds(aligned(b * 256, 256), 256)
        wide = h_ref[r].astype(F32)
        scale = lax.rsqrt(jnp.mean(wide * wide, -1, keepdims=True) + 1e-6)
        a = wide * scale
        a_ref[r] = a.astype(BF16)
        if turned:
            at_ref[:, r] = a.T.astype(BF16)
        return 0

    def gates(r, slot):
        gu = dot(a_ref[r], wgu_buf[slot])
        gate, up = gu[:, :WIDE], gu[:, WIDE:]
        sig = jax.nn.sigmoid(gate)
        return gate * sig, up, sig

    load_x.wait()
    lax.fori_loop(0, tokens // 256, functools.partial(normalise, turned=False), 0)
    acc_ref[...] = jnp.zeros_like(acc_ref)

    def forward(g, _):
        slot = lax.rem(g, 2)
        fetch(g + 1)
        fetched(g)
        for b in range(4):
            r = pl.ds(b * block, block)
            silu, up, _ = gates(r, slot)
            acc_ref[r] += dot((silu * up).astype(BF16), wd_buf[slot])
        return 0

    lax.fori_loop(0, per_layer, forward, 0)

    def join(b, _):
        r = pl.ds(aligned(b * 256, 256), 256)
        h_ref[r] = h_ref[r] + acc_ref[r].astype(BF16)
        acc_ref[r] = jnp.zeros((256, d), F32)
        return normalise(b, 0)

    lax.fori_loop(0, tokens // 256, join, 0)
    load_dy.wait()
    pl.semaphore_wait(barrier, 2)
    for c in moments:
        c.start()

    def backward(t, _, with_da, last):
        g = t + per_layer
        slot = lax.rem(g, 2)
        if last:

            @pl.when(t < tiles - 1)
            def _():
                fetch(g + 1)
        else:
            fetch(g + 1)
        fetched(g)
        lay, j, i = place(t)
        if with_da:

            @pl.when(t == 2)
            def _():
                for c in moments:
                    c.wait()

        def rows_of(b):
            r = pl.ds(b * block, block)
            silu, up, sig = gates(r, slot)
            dp = dot(ct_ref[r], wd_buf[slot], ((1,), (1,))).astype(BF16).astype(F32)
            p_ref[r] = (silu * up).astype(BF16)
            dgu_ref[r, WIDE:] = (dp * silu).astype(BF16)
            dgu_ref[r, :WIDE] = (dp * up * (sig + silu * (1 - sig))).astype(BF16)

        def da(b):
            if with_da:
                r = pl.ds(b * block, block)
                acc_ref[r] += dot(dgu_ref[r], wgu_buf[slot], ((1,), (1,)))

        def up_and_gate(e):
            g_gu[lax.rem(t, SLOTS), e] = dot(at_ref[...], dgu_ref[:, e * WIDE : (e + 1) * WIDE]).astype(BF16)

        def down():
            grads = dot(p_ref[...], ct_ref[...], ((0,), (0,))).astype(BF16)
            for k in range(2):
                g_dn[lax.rem(lax.div(t, per_chunk), DN_SLOTS), 2 * i + k] = grads[k * STRIP : (k + 1) * STRIP]

        work = [functools.partial(rows_of, b) for b in range(4)]
        work += [functools.partial(up_and_gate, 0), functools.partial(up_and_gate, 1), down]
        work += [functools.partial(da, b) for b in range(4)]
        for step in range(STEPS):
            pump(t, step)
            for k in GROUPS[step]:
                work[k]()
        return 0

    lax.fori_loop(0, per_layer, functools.partial(backward, with_da=True, last=False), 0)

    def turn(b, _):
        r = pl.ds(aligned(b * 256, 256), 256)
        wide = h_ref[r].astype(F32)
        scale = lax.rsqrt(jnp.mean(wide * wide, -1, keepdims=True) + 1e-6)
        da = acc_ref[r].astype(BF16).astype(F32)
        inner = jnp.mean(da * wide, -1, keepdims=True)
        ct_ref[r] = ct_ref[r] + (da * scale - wide * (scale * scale * scale * inner)).astype(BF16)
        return 0

    lax.fori_loop(0, tokens // 256, turn, 0)
    load_x.start()
    load_x.wait()
    lax.fori_loop(0, tokens // 256, normalise, 0)
    lax.fori_loop(per_layer, tiles, functools.partial(backward, with_da=False, last=True), 0)

    def drain(t, _):
        for step in range(STEPS):
            pump(t, step)
            event = STEPS * (t - tiles) + step

            @pl.when(event < DRAIN_UNITS * longer)
            def _():
                ag_event(lax.rem(event, DRAIN_UNITS), lax.div(event, DRAIN_UNITS))

        return 0

    drained = (STEPS * (tiles - 1) + DN_FROM + LAG * longer) // STEPS + 1
    lax.fori_loop(tiles, drained, drain, 0)

    def rest(event, _):
        units = 2 * chunks - DRAIN_UNITS
        ag_event(DRAIN_UNITS + lax.rem(event, units), lax.div(event, units))
        return 0

    lax.fori_loop(0, (2 * chunks - DRAIN_UNITS) * longer, rest, 0)

    def last(c, _):
        for e in range(2):
            for direction in range(2):
                new_ended(c, e, direction, length(e, direction) - 1)
        return 0

    lax.fori_loop(0, chunks, last, 0)


def put(*refs):
    *pairs, sem = refs
    copies = [pltpu.make_async_copy(a, b, sem.at[k]) for k, (a, b) in enumerate(zip(pairs[:9], pairs[9:]))]
    for c in copies:
        c.start()
    for c in copies:
        c.wait()


def device_step(n, x, dy, *arrays):
    w, m, v = (arrays[i : i + 3] for i in (0, 3, 6))
    layers, d, ff = w[0].shape
    tokens = x.shape[1]
    rows, share = d // n, ff // n
    hops, chunks = n // 2, share // STRIP * layers
    anywhere = pl.BlockSpec(memory_space=pl.ANY)
    dma = pltpu.SemaphoreType.DMA
    made = pl.pallas_call(
        functools.partial(kernel, n),
        name="step",
        out_shape=[pltpu.VMEM(a.shape, a.dtype) for a in (*w, *m, *v)],
        in_specs=[anywhere] * 11,
        out_specs=[pl.BlockSpec(memory_space=pltpu.VMEM)] * 9,
        scratch_shapes=[
            pltpu.VMEM((tokens, d), BF16),
            pltpu.VMEM((tokens, d), BF16),
            pltpu.VMEM((d, tokens), BF16),
            pltpu.VMEM((tokens, d), BF16),
            pltpu.VMEM((tokens, d), F32),
            pltpu.VMEM((tokens, WIDE), BF16),
            pltpu.VMEM((tokens, 2 * WIDE), BF16),
            pltpu.VMEM((2, d, 2 * WIDE), BF16),
            pltpu.VMEM((2, WIDE, d), BF16),
            pltpu.VMEM((SLOTS, 2, d, WIDE), BF16),
            pltpu.VMEM((DN_SLOTS, n, STRIP, d), BF16),
            pltpu.VMEM((SLOTS, 2, 2, hops, rows, WIDE), BF16),
            pltpu.VMEM((DN_SLOTS, 2, 2, hops, STRIP // 2, d), BF16),
            dma((2, 6)),
            dma((11,)),
            dma((SLOTS, 2, 2)),
            dma((SLOTS, 2, 2, hops)),
            dma((DN_SLOTS, 2, 2)),
            dma((DN_SLOTS, 2, 2, hops)),
            dma((chunks, 2, 2)),
            dma((chunks, 2, 2, hops)),
        ],
        compiler_params=pltpu.CompilerParams(collective_id=0, has_side_effects=True, vmem_limit_bytes=33 * 2**20),
    )(x, dy, *arrays)
    return pl.pallas_call(
        put,
        name="put",
        out_shape=[jax.ShapeDtypeStruct(a.shape, a.dtype) for a in made],
        in_specs=[pl.BlockSpec(memory_space=pltpu.VMEM)] * 9,
        out_specs=[anywhere] * 9,
        scratch_shapes=[dma((9,))],
        compiler_params=pltpu.CompilerParams(vmem_limit_bytes=2**20),
    )(*(pltpu.with_memory_space_constraint(a, pltpu.VMEM) for a in made))


def solution(mesh):
    whole, rows, seq = P(None, None, None), P(None, "dp", None), P(("rep", "dp"), None, None)
    return jax.shard_map(
        functools.partial(device_step, mesh.shape["dp"]),
        mesh=mesh,
        in_specs=(seq, seq) + (whole,) * 3 + (rows,) * 6,
        out_specs=(P("rep", None, None),) * 3 + (P("rep", "dp", None),) * 6,
        check_vma=False,
    )
```

```python
import functools

import jax
import jax.numpy as jnp
from jax import lax
from jax.experimental import pallas as pl
from jax.experimental.pallas import tpu as pltpu
from jax.sharding import PartitionSpec as P

F32 = jnp.float32
BF16 = jnp.bfloat16
MESH = pl.DeviceIdType.MESH
STRIP = 128
WIDE = 2 * STRIP
SLOTS = 6
DN_SLOTS = 3
DRAIN_UNITS = 4
LAG = 4
GROUPS = ((0, 1, 2, 3), (4, 5), (6, 7, 8, 9, 10))
STEPS = len(GROUPS)
GU_FROM = 2
DN_FROM = 3


def dot(a, b, dims=((1,), (0,))):
    return lax.dot_general(a, b, (dims, ((), ())), preferred_element_type=F32)


def aligned(i, m):
    return pl.multiple_of(i, m)


def kernel(
    n, x, dy, wg, wu, wd, mg, mu, md, vg, vu, vd,
    og, ou, od, omg, omu, omd, ovg, ovu, ovd,
    h_ref, a_ref, at_ref, ct_ref, acc_ref, p_ref, dgu_ref, wgu_buf, wd_buf,
    g_gu, g_dn, land_gu, land_dn,
    w_sem, in_sem, gu_send, gu_recv, dn_send, dn_recv, ag_send, ag_recv,
):
    tokens, d = h_ref.shape
    layers, _, ff = wg.shape
    rows = d // n
    share = ff // n
    per_layer = ff // WIDE
    per_chunk = n // 2
    chunks = layers * per_layer // per_chunk
    tiles = layers * per_layer
    half = STRIP // 2
    block = tokens // 4
    few = min(block, 256)
    me, rep = lax.axis_index("dp"), lax.axis_index("rep")
    right, left = lax.rem(me + 1, n), lax.rem(me + n - 1, n)
    to = (right, left)

    longer = n // 2

    def length(e, direction):
        return longer if e == direction else n - 1 - longer

    def owner(e, direction, hop):
        away = length(e, direction) - hop
        return lax.rem(me + away, n) if direction == 0 else lax.rem(me + n - away, n)

    def holder(direction, hop):
        return lax.rem(me + n - hop, n) if direction == 0 else lax.rem(me + hop, n)

    def place(t):
        tt = lax.rem(t, per_layer)
        return layers - 1 - lax.div(t, per_layer), lax.div(tt, per_chunk), lax.rem(tt, per_chunk)

    def strips(j, i):
        return [aligned((2 * i + k) * share + STRIP * j, STRIP) for k in range(2)]

    def tile_copies(g):
        lay = lax.rem(lax.div(g, per_layer), 2)
        tt = lax.rem(g, per_layer)
        cols = strips(lax.div(tt, per_chunk), lax.rem(tt, per_chunk))
        slot = lax.rem(g, 4)
        out = []
        for k, col in enumerate(cols):
            strip = pl.ds(col, STRIP)
            for q, w in enumerate((wg, wu)):
                out.append((w.at[lay, :, strip], wgu_buf.at[slot, :, pl.ds(q * WIDE + k * STRIP, STRIP)]))
            out.append((wd.at[lay, strip], wd_buf.at[slot, pl.ds(k * STRIP, STRIP)]))
        return [pltpu.make_async_copy(a, b, w_sem.at[slot, k]) for k, (a, b) in enumerate(out)]

    def fetch(g):
        for c in tile_copies(g):
            c.start()

    def fetched(g):
        for c in tile_copies(g):
            c.wait()

    parts = [pl.ds(b * block, block) for b in range(4)]
    load_x = [pltpu.make_async_copy(x.at[0, r], h_ref.at[r], in_sem.at[11 + b]) for b, r in enumerate(parts)]
    load_dy = pltpu.make_async_copy(dy.at[0], ct_ref, in_sem.at[1])
    my_rows, my_share = pl.ds(aligned(me * rows, rows), rows), pl.ds(aligned(me * share, share), share)
    moments = [
        pltpu.make_async_copy(a, b, in_sem.at[2 + k])
        for k, (a, b) in enumerate(
            ((mg, omg), (mu, omu), (md, omd), (vg, ovg), (vu, ovu), (vd, ovd),
             (wg.at[:, my_rows], og.at[:, my_rows]), (wu.at[:, my_rows], ou.at[:, my_rows]), (wd.at[:, my_share], od.at[:, my_share]))
        )
    ]

    barrier = pltpu.get_barrier_semaphore()
    for other in to:
        pl.semaphore_signal(barrier, inc=1, device_id=(rep, other), device_id_type=MESH)
    for c in load_x:
        c.start()
    fetch(0)
    fetch(1)
    load_dy.start()

    def remote(src, dst, send, recv, direction):
        return pltpu.make_async_remote_copy(
            src_ref=src, dst_ref=dst, send_sem=send, recv_sem=recv, device_id=(rep, to[direction]), device_id_type=MESH
        )

    def adam(w, m, v, g):
        g = g.astype(F32)
        m = 0.9 * m + 0.1 * g
        v = 0.95 * v + 0.05 * g * g
        step = m * lax.rsqrt(v + 1e-8) + 0.1 * w
        return (w - 0.02 * step).astype(BF16), m, v

    def sum_event(hop, own, land, send, recv, update):
        def copy(e, direction, h):
            src = own(e, owner(e, direction, 0)) if h == 0 else land.at[e, direction, h - 1]
            return remote(src, land.at[e, direction, h], send.at[e, direction], recv.at[e, direction, h], direction)

        def ended(e, direction, h):
            before = copy(e, direction, h)
            before.wait_send()
            before.wait_recv()
            return land[e, direction, h].astype(F32)

        if hop == longer:
            for e in range(2):
                whole = own(e, me)[...].astype(F32)
                for direction in range(2):
                    whole += ended(e, direction, length(e, direction) - 1)
                update(e, whole.astype(BF16))
            return
        ready = []
        for e, direction in ((0, 0), (1, 1), (1, 0), (0, 1)):
            if hop >= length(e, direction):
                continue
            if hop > 0:
                mine = own(e, owner(e, direction, hop))[...].astype(F32)
                land[e, direction, hop - 1] = (ended(e, direction, hop - 1) + mine).astype(BF16)
            ready.append(copy(e, direction, hop))
            if len(ready) > 1:
                ready[-2].start()
        ready[-1].start()

    def gu_event(u, hop):
        slot = lax.rem(u, SLOTS)
        lay, j, i = place(u)

        def update(e, g):
            w, m, v = ((og, omg, ovg), (ou, omu, ovu))[e]
            for k, col in enumerate(strips(j, i)):
                strip = pl.ds(col, STRIP)
                w[lay, my_rows, strip], m[lay, :, strip], v[lay, :, strip] = adam(
                    w[lay, my_rows, strip].astype(F32), m[lay, :, strip], v[lay, :, strip], g[:, k * STRIP : (k + 1) * STRIP]
                )

        def own(e, who):
            return g_gu.at[slot, e, pl.ds(aligned(who * rows, rows), rows)]

        sum_event(hop, own, land_gu.at[slot], gu_send.at[slot], gu_recv.at[slot], update)

    def dn_event(c, hop):
        slot, there = lax.rem(c, DN_SLOTS), lax.rem(c, 2)
        lay, j, _ = place(c * per_chunk)

        def update(e, g):
            r = pl.ds(aligned(STRIP * j + e * half, half), half)
            mine = pl.ds(aligned(me * share + STRIP * j + e * half, half), half)
            od[lay, mine], omd[lay, r], ovd[lay, r] = adam(od[lay, mine].astype(F32), omd[lay, r], ovd[lay, r], g)

        def own(e, who):
            return g_dn.at[slot, who, pl.ds(e * half, half)]

        sum_event(hop, own, land_dn.at[there], dn_send.at[there], dn_recv.at[there], update)

    def new_copies(c, e, direction, h):
        lay, j, _ = place(c * per_chunk)
        who = holder(direction, h)
        send, recv = ag_send.at[c, e, direction], ag_recv.at[c, e, direction, h]
        out, r = (og, ou)[e], pl.ds(aligned(who * rows, rows), rows)

        for i in range(n):
            there = out.at[lay, r, pl.ds(aligned(i * share + STRIP * j, STRIP), STRIP)]
            remote(there, there, send, recv, direction).start()
        there = od.at[lay, pl.ds(aligned(who * share + STRIP * j + e * half, half), half)]
        remote(there, there, send, recv, direction).start()

    def new_ended(c, e, direction, h):
        sent = (n * rows * STRIP + half * d) // d
        all_of_it = od.at[0, pl.ds(0, sent)]
        before = remote(all_of_it, all_of_it, ag_send.at[c, e, direction], ag_recv.at[c, e, direction, h], direction)
        before.wait_send()
        before.wait_recv()

    def ag_event(unit, hop):
        c = lax.div(unit, 2)
        for e in range(2):

            @pl.when(lax.rem(unit, 2) == e)
            def _():
                for direction in range(2):

                    @pl.when((hop > 0) & (hop < length(e, direction)))
                    def _():
                        new_ended(c, e, direction, hop - 1)

                for direction in range(2):

                    @pl.when(hop < length(e, direction))
                    def _():
                        new_copies(c, e, direction, hop)

    def pump(t, step):
        for hop in range(longer + 1):
            since, due = divmod(GU_FROM + LAG * hop, STEPS)
            if due == step:

                @pl.when((t >= since) & (t < tiles + since))
                def _():
                    gu_event(t - since, hop)

            since, due = divmod(DN_FROM + LAG * hop, STEPS)
            if due == step:

                @pl.when((t >= since) & (t < tiles + since) & (lax.rem(t - since + 1, per_chunk) == 0))
                def _():
                    dn_event(lax.div(t - since, per_chunk), hop)

    def normalise(b, _, turned=True):
        r = pl.ds(aligned(b * few, few), few)
        wide = h_ref[r].astype(F32)
        scale = lax.rsqrt(jnp.mean(wide * wide, -1, keepdims=True) + 1e-6)
        a = wide * scale
        a_ref[r] = a.astype(BF16)
        if turned:
            at_ref[:, r] = a.T.astype(BF16)
        return 0

    def gates(r, slot):
        gu = dot(a_ref[r], wgu_buf[slot])
        gate, up = gu[:, :WIDE], gu[:, WIDE:]
        sig = jax.nn.sigmoid(gate)
        return gate * sig, up, sig

    def each(b, do):
        for k in range(block // few):
            do(b * (block // few) + k, 0)

    def forward(pair, _, first=False):
        g = 2 * pair
        slot = lax.rem(g, 4)
        for k in range(2):
            fetch(g + 2 + k)
            fetched(g + k)
        for b in range(4):
            r = pl.ds(b * block, block)
            if first:
                load_x[b].wait()
                each(b, functools.partial(normalise, turned=False))
            act = []
            for k in range(2):
                silu, up, _ = gates(r, slot + k)
                act.append((silu * up).astype(BF16))
            part = dot(jnp.concatenate(act, 1), wd_buf[pl.ds(slot, 2)].reshape(2 * WIDE, d))
            acc_ref[r] = part if first else acc_ref[r] + part
        return 0

    forward(0, 0, first=True)
    lax.fori_loop(1, per_layer // 2, forward, 0)

    def join(b, _):
        r = pl.ds(aligned(b * few, few), few)
        h_ref[r] = h_ref[r] + acc_ref[r].astype(BF16)
        return normalise(b, 0)

    load_dy.wait()
    pl.semaphore_wait(barrier, 2)
    for c in moments:
        c.start()

    def backward(t, _, with_da, last, first=False):
        g = t + per_layer
        slot = lax.rem(g, 4)
        if last:

            @pl.when(t < tiles - 2)
            def _():
                fetch(g + 2)
        else:
            fetch(g + 2)
        fetched(g)
        lay, j, i = place(t)
        if with_da and not first:

            @pl.when(t == 2)
            def _():
                for c in moments:
                    c.wait()

        def rows_of(b):
            r = pl.ds(b * block, block)
            if first:
                each(b, join)
            silu, up, sig = gates(r, slot)
            dp = dot(ct_ref[r], wd_buf[slot], ((1,), (1,))).astype(BF16).astype(F32)
            p_ref[r] = (silu * up).astype(BF16)
            dgu_ref[r, WIDE:] = (dp * silu).astype(BF16)
            dgu_ref[r, :WIDE] = (dp * up * (sig + silu * (1 - sig))).astype(BF16)

        def da(b):
            if with_da:
                r = pl.ds(b * block, block)
                part = dot(dgu_ref[r], wgu_buf[slot], ((1,), (1,)))
                acc_ref[r] = part if first else acc_ref[r] + part

        def up_and_gate(e):
            g_gu[lax.rem(t, SLOTS), e] = dot(at_ref[...], dgu_ref[:, e * WIDE : (e + 1) * WIDE]).astype(BF16)

        def down():
            grads = dot(p_ref[...], ct_ref[...], ((0,), (0,))).astype(BF16)
            for k in range(2):
                g_dn[lax.rem(lax.div(t, per_chunk), DN_SLOTS), 2 * i + k] = grads[k * STRIP : (k + 1) * STRIP]

        work = [functools.partial(rows_of, b) for b in range(4)]
        work += [functools.partial(up_and_gate, 0), functools.partial(up_and_gate, 1), down]
        work += [functools.partial(da, b) for b in range(4)]
        for step in range(STEPS):
            if not first:
                pump(t, step)
            elif step == GU_FROM:
                gu_event(0, 0)
            for k in GROUPS[step]:
                work[k]()
        return 0

    backward(0, 0, with_da=True, last=False, first=True)
    lax.fori_loop(1, per_layer, functools.partial(backward, with_da=True, last=False), 0)

    def turn(b, _):
        r = pl.ds(aligned(b * few, few), few)
        wide = h_ref[r].astype(F32)
        scale = lax.rsqrt(jnp.mean(wide * wide, -1, keepdims=True) + 1e-6)
        da = acc_ref[r].astype(BF16).astype(F32)
        inner = jnp.mean(da * wide, -1, keepdims=True)
        ct_ref[r] = ct_ref[r] + (da * scale - wide * (scale * scale * scale * inner)).astype(BF16)
        return 0

    lax.fori_loop(0, tokens // few, turn, 0)
    for c in load_x:
        c.start()
    for c in load_x:
        c.wait()
    lax.fori_loop(0, tokens // few, normalise, 0)
    lax.fori_loop(per_layer, tiles, functools.partial(backward, with_da=False, last=True), 0)

    def drain(t, _):
        for step in range(STEPS):
            pump(t, step)
            event = STEPS * (t - tiles) + step

            @pl.when(event < DRAIN_UNITS * longer)
            def _():
                ag_event(lax.rem(event, DRAIN_UNITS), lax.div(event, DRAIN_UNITS))

        return 0

    drained = (STEPS * (tiles - 1) + DN_FROM + LAG * longer) // STEPS + 1
    lax.fori_loop(tiles, drained, drain, 0)
    def rest(event, _):
        units = 2 * chunks - DRAIN_UNITS
        ag_event(DRAIN_UNITS + lax.rem(event, units), lax.div(event, units))
        return 0

    lax.fori_loop(0, (2 * chunks - DRAIN_UNITS) * longer, rest, 0)

    def last(c, _):
        for e in range(2):
            for direction in range(2):
                new_ended(c, e, direction, length(e, direction) - 1)
        return 0

    lax.fori_loop(0, chunks, last, 0)


def put(*refs):
    *pairs, sem = refs
    copies = []
    for k, (a, b) in enumerate(zip(pairs[:9], pairs[9:])):
        for lay in range(a.shape[0]):
            copies.append(pltpu.make_async_copy(a.at[lay], b.at[lay], sem.at[k, lay]))
    for c in copies:
        c.start()
    for c in copies:
        c.wait()


def device_step(n, x, dy, *arrays):
    w, m, v = (arrays[i : i + 3] for i in (0, 3, 6))
    layers, d, ff = w[0].shape
    tokens = x.shape[1]
    rows, share = d // n, ff // n
    hops, chunks = n // 2, share // STRIP * layers
    anywhere = pl.BlockSpec(memory_space=pl.ANY)
    dma = pltpu.SemaphoreType.DMA
    made = pl.pallas_call(
        functools.partial(kernel, n),
        name="step",
        out_shape=[pltpu.VMEM(a.shape, a.dtype) for a in (*w, *m, *v)],
        in_specs=[anywhere] * 11,
        out_specs=[pl.BlockSpec(memory_space=pltpu.VMEM)] * 9,
        scratch_shapes=[
            pltpu.VMEM((tokens, d), BF16),
            pltpu.VMEM((tokens, d), BF16),
            pltpu.VMEM((d, tokens), BF16),
            pltpu.VMEM((tokens, d), BF16),
            pltpu.VMEM((tokens, d), F32),
            pltpu.VMEM((tokens, WIDE), BF16),
            pltpu.VMEM((tokens, 2 * WIDE), BF16),
            pltpu.VMEM((4, d, 2 * WIDE), BF16),
            pltpu.VMEM((4, WIDE, d), BF16),
            pltpu.VMEM((SLOTS, 2, d, WIDE), BF16),
            pltpu.VMEM((DN_SLOTS, n, STRIP, d), BF16),
            pltpu.VMEM((SLOTS, 2, 2, hops, rows, WIDE), BF16),
            pltpu.VMEM((2, 2, 2, hops, STRIP // 2, d), BF16),
            dma((4, 6)),
            dma((15,)),
            dma((SLOTS, 2, 2)),
            dma((SLOTS, 2, 2, hops)),
            dma((2, 2, 2)),
            dma((2, 2, 2, hops)),
            dma((chunks, 2, 2)),
            dma((chunks, 2, 2, hops)),
        ],
        compiler_params=pltpu.CompilerParams(collective_id=0, has_side_effects=True, vmem_limit_bytes=73 * 2**19),
    )(x, dy, *arrays)
    return pl.pallas_call(
        put,
        name="put",
        out_shape=[jax.ShapeDtypeStruct(a.shape, a.dtype) for a in made],
        in_specs=[pl.BlockSpec(memory_space=pltpu.VMEM)] * 9,
        out_specs=[anywhere] * 9,
        scratch_shapes=[dma((9, layers))],
        compiler_params=pltpu.CompilerParams(vmem_limit_bytes=2**20),
    )(*(pltpu.with_memory_space_constraint(a, pltpu.VMEM) for a in made))


def solution(mesh):
    whole, rows, seq = P(None, None, None), P(None, "dp", None), P(("rep", "dp"), None, None)
    return jax.shard_map(
        functools.partial(device_step, mesh.shape["dp"]),
        mesh=mesh,
        in_specs=(seq, seq) + (whole,) * 3 + (rows,) * 6,
        out_specs=(P("rep", None, None),) * 3 + (P("rep", "dp", None),) * 6,
        check_vma=False,
    )
```

```python
import functools

import jax
import jax.numpy as jnp
from jax import lax
from jax.experimental import pallas as pl
from jax.experimental.pallas import tpu as pltpu
from jax.sharding import PartitionSpec as P

F32 = jnp.float32
BF16 = jnp.bfloat16
MESH = pl.DeviceIdType.MESH
STRIP = 128
WIDE = 2 * STRIP
SLOTS = 6
DN_SLOTS = 3
DRAIN_UNITS = 4
LAG = 4
GROUPS = ((0, 1, 2, 3), (4, 5), (6, 7, 8, 9, 10))
STEPS = len(GROUPS)
GU_FROM = 2
DN_FROM = 3
EARLY = 4
EARLY_LAG = 3


def dot(a, b, dims=((1,), (0,))):
    return lax.dot_general(a, b, (dims, ((), ())), preferred_element_type=F32)


def aligned(i, m):
    return pl.multiple_of(i, m)


def kernel(
    n, x, dy, wg, wu, wd, mg, mu, md, vg, vu, vd,
    og, ou, od, omg, omu, omd, ovg, ovu, ovd,
    h_ref, a_ref, at_ref, ct_ref, acc_ref, p_ref, dgu_ref, wgu_buf, wd_buf,
    g_gu, g_dn, land_gu, land_dn,
    w_sem, in_sem, gu_send, gu_recv, dn_send, dn_recv, ag_send, ag_recv,
):
    tokens, d = h_ref.shape
    layers, _, ff = wg.shape
    rows = d // n
    share = ff // n
    per_layer = ff // WIDE
    per_chunk = n // 2
    chunks = layers * per_layer // per_chunk
    tiles = layers * per_layer
    half = STRIP // 2
    block = tokens // 4
    few = min(block, 256)
    me, rep = lax.axis_index("dp"), lax.axis_index("rep")
    right, left = lax.rem(me + 1, n), lax.rem(me + n - 1, n)
    to = (right, left)

    longer = n // 2

    def length(e, direction):
        return longer if e == direction else n - 1 - longer

    def owner(e, direction, hop):
        away = length(e, direction) - hop
        return lax.rem(me + away, n) if direction == 0 else lax.rem(me + n - away, n)

    def holder(direction, hop):
        return lax.rem(me + n - hop, n) if direction == 0 else lax.rem(me + hop, n)

    def place(t):
        tt = lax.rem(t, per_layer)
        return layers - 1 - lax.div(t, per_layer), lax.div(tt, per_chunk), lax.rem(tt, per_chunk)

    def strips(j, i):
        return [aligned((2 * i + k) * share + STRIP * j, STRIP) for k in range(2)]

    def tile_copies(g):
        lay = lax.rem(lax.div(g, per_layer), 2)
        tt = lax.rem(g, per_layer)
        cols = strips(lax.div(tt, per_chunk), lax.rem(tt, per_chunk))
        slot = lax.rem(g, 4)
        out = []
        for k, col in enumerate(cols):
            strip = pl.ds(col, STRIP)
            for q, w in enumerate((wg, wu)):
                out.append((w.at[lay, :, strip], wgu_buf.at[slot, :, pl.ds(q * WIDE + k * STRIP, STRIP)]))
            out.append((wd.at[lay, strip], wd_buf.at[slot, pl.ds(k * STRIP, STRIP)]))
        return [pltpu.make_async_copy(a, b, w_sem.at[slot, k]) for k, (a, b) in enumerate(out)]

    def fetch(g):
        for c in tile_copies(g):
            c.start()

    def fetched(g):
        for c in tile_copies(g):
            c.wait()

    parts = [pl.ds(b * block, block) for b in range(4)]
    load_x = [pltpu.make_async_copy(x.at[0, r], h_ref.at[r], in_sem.at[11 + b]) for b, r in enumerate(parts)]
    load_dy = pltpu.make_async_copy(dy.at[0], ct_ref, in_sem.at[1])
    my_rows, my_share = pl.ds(aligned(me * rows, rows), rows), pl.ds(aligned(me * share, share), share)
    moments = [
        pltpu.make_async_copy(a, b, in_sem.at[2 + k])
        for k, (a, b) in enumerate(
            ((mg, omg), (mu, omu), (md, omd), (vg, ovg), (vu, ovu), (vd, ovd),
             (wg.at[:, my_rows], og.at[:, my_rows]), (wu.at[:, my_rows], ou.at[:, my_rows]), (wd.at[:, my_share], od.at[:, my_share]))
        )
    ]

    barrier = pltpu.get_barrier_semaphore()
    for other in to:
        pl.semaphore_signal(barrier, inc=1, device_id=(rep, other), device_id_type=MESH)
    for c in load_x:
        c.start()
    fetch(0)
    fetch(1)
    load_dy.start()

    def remote(src, dst, send, recv, direction):
        return pltpu.make_async_remote_copy(
            src_ref=src, dst_ref=dst, send_sem=send, recv_sem=recv, device_id=(rep, to[direction]), device_id_type=MESH
        )

    def adam(w, m, v, g):
        g = g.astype(F32)
        m = 0.9 * m + 0.1 * g
        v = 0.95 * v + 0.05 * g * g
        step = m * lax.rsqrt(v + 1e-8) + 0.1 * w
        return (w - 0.02 * step).astype(BF16), m, v

    def sum_event(hop, own, land, send, recv, update):
        def copy(e, direction, h):
            src = own(e, owner(e, direction, 0)) if h == 0 else land.at[e, direction, h - 1]
            return remote(src, land.at[e, direction, h], send.at[e, direction], recv.at[e, direction, h], direction)

        def ended(e, direction, h):
            before = copy(e, direction, h)
            before.wait_send()
            before.wait_recv()
            return land[e, direction, h].astype(F32)

        if hop == longer:
            for e in range(2):
                whole = own(e, me)[...].astype(F32)
                for direction in range(2):
                    whole += ended(e, direction, length(e, direction) - 1)
                update(e, whole.astype(BF16))
            return
        ready = []
        for e, direction in ((0, 0), (1, 1), (1, 0), (0, 1)):
            if hop >= length(e, direction):
                continue
            if hop > 0:
                mine = own(e, owner(e, direction, hop))[...].astype(F32)
                land[e, direction, hop - 1] = (ended(e, direction, hop - 1) + mine).astype(BF16)
            ready.append(copy(e, direction, hop))
            if len(ready) > 1:
                ready[-2].start()
        ready[-1].start()

    def gu_event(u, hop):
        slot = lax.rem(u, SLOTS)
        lay, j, i = place(u)

        def update(e, g):
            w, m, v = ((og, omg, ovg), (ou, omu, ovu))[e]
            for k, col in enumerate(strips(j, i)):
                strip = pl.ds(col, STRIP)
                w[lay, my_rows, strip], m[lay, :, strip], v[lay, :, strip] = adam(
                    w[lay, my_rows, strip].astype(F32), m[lay, :, strip], v[lay, :, strip], g[:, k * STRIP : (k + 1) * STRIP]
                )

        def own(e, who):
            return g_gu.at[slot, e, pl.ds(aligned(who * rows, rows), rows)]

        sum_event(hop, own, land_gu.at[slot], gu_send.at[slot], gu_recv.at[slot], update)

    def dn_event(c, hop):
        slot, there = lax.rem(c, DN_SLOTS), lax.rem(c, 2)
        lay, j, _ = place(c * per_chunk)

        def update(e, g):
            r = pl.ds(aligned(STRIP * j + e * half, half), half)
            mine = pl.ds(aligned(me * share + STRIP * j + e * half, half), half)
            od[lay, mine], omd[lay, r], ovd[lay, r] = adam(od[lay, mine].astype(F32), omd[lay, r], ovd[lay, r], g)

        def own(e, who):
            return g_dn.at[slot, who, pl.ds(e * half, half)]

        sum_event(hop, own, land_dn.at[there], dn_send.at[there], dn_recv.at[there], update)

    def new_copies(c, e, direction, h):
        lay, j, _ = place(c * per_chunk)
        who = holder(direction, h)
        send, recv = ag_send.at[c, e, direction], ag_recv.at[c, e, direction, h]
        out, r = (og, ou)[e], pl.ds(aligned(who * rows, rows), rows)

        for i in range(n):
            there = out.at[lay, r, pl.ds(aligned(i * share + STRIP * j, STRIP), STRIP)]
            remote(there, there, send, recv, direction).start()
        there = od.at[lay, pl.ds(aligned(who * share + STRIP * j + e * half, half), half)]
        remote(there, there, send, recv, direction).start()

    def new_ended(c, e, direction, h):
        sent = (n * rows * STRIP + half * d) // d
        all_of_it = od.at[0, pl.ds(0, sent)]
        before = remote(all_of_it, all_of_it, ag_send.at[c, e, direction], ag_recv.at[c, e, direction, h], direction)
        before.wait_send()
        before.wait_recv()

    def ag_event(unit, hop):
        c = lax.div(unit, 2)
        for e in range(2):

            @pl.when(lax.rem(unit, 2) == e)
            def _():
                for direction in range(2):

                    @pl.when((hop > 0) & (hop < length(e, direction)))
                    def _():
                        new_ended(c, e, direction, hop - 1)

                    @pl.when(hop < length(e, direction))
                    def _():
                        new_copies(c, e, direction, hop)

    def pump(t, step, early=False):
        groups = [(LAG, EARLY, tiles)]
        if early:
            groups.insert(0, (EARLY_LAG, 0, EARLY))
        for lag, begin, end in groups:
            for hop in range(longer + 1):
                since, due = divmod(GU_FROM + lag * hop, STEPS)
                if due == step:

                    @pl.when((t >= begin + since) & (t < end + since))
                    def _():
                        gu_event(t - since, hop)

                since, due = divmod(DN_FROM + lag * hop, STEPS)
                if due == step:

                    @pl.when((t >= begin + since) & (t < end + since) & (lax.rem(t - since + 1, per_chunk) == 0))
                    def _():
                        dn_event(lax.div(t - since, per_chunk), hop)

    def normalise(b, _, turned=True):
        r = pl.ds(aligned(b * few, few), few)
        wide = h_ref[r].astype(F32)
        scale = lax.rsqrt(jnp.mean(wide * wide, -1, keepdims=True) + 1e-6)
        a = wide * scale
        a_ref[r] = a.astype(BF16)
        if turned:
            at_ref[:, r] = a.T.astype(BF16)
        return 0

    def gates(r, slot):
        gu = dot(a_ref[r], wgu_buf[slot])
        gate, up = gu[:, :WIDE], gu[:, WIDE:]
        sig = jax.nn.sigmoid(gate)
        return gate * sig, up, sig

    def each(b, do):
        for k in range(block // few):
            do(b * (block // few) + k, 0)

    def forward(pair, _, first=False):
        g = 2 * pair
        slot = lax.rem(g, 4)
        for k in range(2):
            fetch(g + 2 + k)
            fetched(g + k)
        for b in range(4):
            r = pl.ds(b * block, block)
            if first:
                load_x[b].wait()
                each(b, functools.partial(normalise, turned=False))
            act = []
            for k in range(2):
                silu, up, _ = gates(r, slot + k)
                act.append((silu * up).astype(BF16))
            part = dot(jnp.concatenate(act, 1), wd_buf[pl.ds(slot, 2)].reshape(2 * WIDE, d))
            acc_ref[r] = part if first else acc_ref[r] + part
        return 0

    forward(0, 0, first=True)
    lax.fori_loop(1, per_layer // 2, forward, 0)

    def join(b, _):
        r = pl.ds(aligned(b * few, few), few)
        h_ref[r] = h_ref[r] + acc_ref[r].astype(BF16)
        return normalise(b, 0)

    load_dy.wait()
    pl.semaphore_wait(barrier, 2)
    for c in moments:
        c.start()

    def backward(t, _, with_da, last, first=False):
        g = t + per_layer
        slot = lax.rem(g, 4)
        if last:

            @pl.when(t < tiles - 2)
            def _():
                fetch(g + 2)
        else:
            fetch(g + 2)
        fetched(g)
        lay, j, i = place(t)
        if with_da and not first:

            @pl.when(t == 2)
            def _():
                for c in moments:
                    c.wait()

        def rows_of(b):
            r = pl.ds(b * block, block)
            if first:
                each(b, join)
            silu, up, sig = gates(r, slot)
            dp = dot(ct_ref[r], wd_buf[slot], ((1,), (1,))).astype(BF16).astype(F32)
            p_ref[r] = (silu * up).astype(BF16)
            dgu_ref[r, WIDE:] = (dp * silu).astype(BF16)
            dgu_ref[r, :WIDE] = (dp * up * (sig + silu * (1 - sig))).astype(BF16)

        def da(b):
            if with_da:
                r = pl.ds(b * block, block)
                part = dot(dgu_ref[r], wgu_buf[slot], ((1,), (1,)))
                acc_ref[r] = part if first else acc_ref[r] + part

        def up_and_gate(e):
            g_gu[lax.rem(t, SLOTS), e] = dot(at_ref[...], dgu_ref[:, e * WIDE : (e + 1) * WIDE]).astype(BF16)

        def down():
            grads = dot(p_ref[...], ct_ref[...], ((0,), (0,))).astype(BF16)
            for k in range(2):
                g_dn[lax.rem(lax.div(t, per_chunk), DN_SLOTS), 2 * i + k] = grads[k * STRIP : (k + 1) * STRIP]

        work = [functools.partial(rows_of, b) for b in range(4)]
        work += [functools.partial(up_and_gate, 0), functools.partial(up_and_gate, 1), down]
        work += [functools.partial(da, b) for b in range(4)]
        for step in range(STEPS):
            if not first:
                pump(t, step, with_da)
            elif step == GU_FROM:
                gu_event(0, 0)
            for k in GROUPS[step]:
                work[k]()
        return 0

    backward(0, 0, with_da=True, last=False, first=True)
    lax.fori_loop(1, per_layer, functools.partial(backward, with_da=True, last=False), 0)

    def turn(b, _):
        r = pl.ds(aligned(b * few, few), few)
        wide = h_ref[r].astype(F32)
        scale = lax.rsqrt(jnp.mean(wide * wide, -1, keepdims=True) + 1e-6)
        da = acc_ref[r].astype(BF16).astype(F32)
        inner = jnp.mean(da * wide, -1, keepdims=True)
        ct_ref[r] = ct_ref[r] + (da * scale - wide * (scale * scale * scale * inner)).astype(BF16)
        return 0

    lax.fori_loop(0, tokens // few, turn, 0)
    for c in load_x:
        c.start()
    for c in load_x:
        c.wait()
    lax.fori_loop(0, tokens // few, normalise, 0)
    lax.fori_loop(per_layer, tiles, functools.partial(backward, with_da=False, last=True), 0)

    def drain(t, _):
        for step in range(STEPS):
            pump(t, step)
            event = STEPS * (t - tiles) + step

            @pl.when(event < DRAIN_UNITS * longer)
            def _():
                ag_event(lax.rem(event, DRAIN_UNITS), lax.div(event, DRAIN_UNITS))

        return 0

    drained = (STEPS * (tiles - 1) + DN_FROM + LAG * longer) // STEPS + 1
    lax.fori_loop(tiles, drained, drain, 0)
    def rest(event, _):
        units = 2 * chunks - DRAIN_UNITS
        ag_event(DRAIN_UNITS + lax.rem(event, units), lax.div(event, units))
        return 0

    lax.fori_loop(0, (2 * chunks - DRAIN_UNITS) * longer, rest, 0)

    def last(c, _):
        for e in range(2):
            for direction in range(2):
                new_ended(c, e, direction, length(e, direction) - 1)
        return 0

    lax.fori_loop(0, chunks, last, 0)


def put(*refs):
    *pairs, sem = refs
    copies = []
    for k, (a, b) in enumerate(zip(pairs[:9], pairs[9:])):
        for lay in range(a.shape[0]):
            copies.append(pltpu.make_async_copy(a.at[lay], b.at[lay], sem.at[k, lay]))
    for c in copies:
        c.start()
    for c in copies:
        c.wait()


def device_step(n, x, dy, *arrays):
    w, m, v = (arrays[i : i + 3] for i in (0, 3, 6))
    layers, d, ff = w[0].shape
    tokens = x.shape[1]
    rows, share = d // n, ff // n
    hops, chunks = n // 2, share // STRIP * layers
    anywhere = pl.BlockSpec(memory_space=pl.ANY)
    dma = pltpu.SemaphoreType.DMA
    made = pl.pallas_call(
        functools.partial(kernel, n),
        name="step",
        out_shape=[pltpu.VMEM(a.shape, a.dtype) for a in (*w, *m, *v)],
        in_specs=[anywhere] * 11,
        out_specs=[pl.BlockSpec(memory_space=pltpu.VMEM)] * 9,
        scratch_shapes=[
            pltpu.VMEM((tokens, d), BF16),
            pltpu.VMEM((tokens, d), BF16),
            pltpu.VMEM((d, tokens), BF16),
            pltpu.VMEM((tokens, d), BF16),
            pltpu.VMEM((tokens, d), F32),
            pltpu.VMEM((tokens, WIDE), BF16),
            pltpu.VMEM((tokens, 2 * WIDE), BF16),
            pltpu.VMEM((4, d, 2 * WIDE), BF16),
            pltpu.VMEM((4, WIDE, d), BF16),
            pltpu.VMEM((SLOTS, 2, d, WIDE), BF16),
            pltpu.VMEM((DN_SLOTS, n, STRIP, d), BF16),
            pltpu.VMEM((SLOTS, 2, 2, hops, rows, WIDE), BF16),
            pltpu.VMEM((2, 2, 2, hops, STRIP // 2, d), BF16),
            dma((4, 6)),
            dma((15,)),
            dma((SLOTS, 2, 2)),
            dma((SLOTS, 2, 2, hops)),
            dma((2, 2, 2)),
            dma((2, 2, 2, hops)),
            dma((chunks, 2, 2)),
            dma((chunks, 2, 2, hops)),
        ],
        compiler_params=pltpu.CompilerParams(collective_id=0, has_side_effects=True, vmem_limit_bytes=73 * 2**19),
    )(x, dy, *arrays)
    return pl.pallas_call(
        put,
        name="put",
        out_shape=[jax.ShapeDtypeStruct(a.shape, a.dtype) for a in made],
        in_specs=[pl.BlockSpec(memory_space=pltpu.VMEM)] * 9,
        out_specs=[anywhere] * 9,
        scratch_shapes=[dma((9, layers))],
        compiler_params=pltpu.CompilerParams(vmem_limit_bytes=2**20),
    )(*(pltpu.with_memory_space_constraint(a, pltpu.VMEM) for a in made))


def solution(mesh):
    whole, rows, seq = P(None, None, None), P(None, "dp", None), P(("rep", "dp"), None, None)
    return jax.shard_map(
        functools.partial(device_step, mesh.shape["dp"]),
        mesh=mesh,
        in_specs=(seq, seq) + (whole,) * 3 + (rows,) * 6,
        out_specs=(P("rep", None, None),) * 3 + (P("rep", "dp", None),) * 6,
        check_vma=False,
    )
```
